32 devices in a mesh: dp: 4 (over x, core), mp: 8 (over z, y).
Axes of the slice: x: 2, y: 2, z: 4, core: 2. Of those that a mesh axis runs over, the one named last changes fastest.
Arguments:
- tokens: bfloat16 [3072, 6144], P('dp'), may hold values from -60 to 60
- ln_gain: float32 [6144], replicated, may hold values from 0.1 to 1.9
- w_qkv: bfloat16 [6144, 3, 6144], P('dp', None, 'mp'), may hold values from -1 to 1
- q_gain: float32 [128], replicated, may hold values from 0.7 to 2
- k_gain: float32 [128], replicated, may hold values from 0.7 to 2
Outputs:
- context: bfloat16 [3072, 6144], P('dp', 'mp')
The draws below stay inside these ranges and needn't reach their ends.
All inputs are finite; a program needn't handle non-finite values.
Results may differ from the reference program's by a relative error of at most 0.012.
The reference program's roundings to bfloat16 on the way count: a program that leaves them out, or rounds other values in their place, can miss the bound.
Values may be sent and summed in bfloat16 or wider, within the bound.
A program may use at most 128 MiB of HBM per device.

```python
import jax
import jax.numpy as jnp
from jax import lax

D = 6144
HEADS = 48
HEAD_DIM = 128
PATCHES = 256
SPLITS = 4
IMAGES = 12
TOKENS = 3072


def draw_tokens(key, part):
    subkeys = jax.random.split(key, 3)
    row_scale = jnp.exp(jax.random.uniform(subkeys[0], (TOKENS, 1), jnp.float32, -1.2, 1.2))
    col_scale = jnp.exp(jax.random.uniform(subkeys[1], (1, D), jnp.float32, -1.2, 1.2))
    base_draw = jnp.clip(jax.random.normal(subkeys[2], (TOKENS, D), jnp.float32), -4.0, 4.0)
    values = base_draw * row_scale * col_scale
    return jnp.clip(values, -60.0, 60.0).astype(jnp.bfloat16)


def draw_w_qkv(key, part):
    subkeys = jax.random.split(key, 2)
    col_scale = jnp.exp(jax.random.uniform(subkeys[0], (1, 3, D), jnp.float32, -1.0, 1.2))
    base_draw = jnp.clip(jax.random.normal(subkeys[1], (D, 3, D), jnp.float32), -4.0, 4.0)
    values = base_draw * col_scale * D ** (-0.5)
    return jnp.clip(values, -1.0, 1.0).astype(jnp.bfloat16)


def setup_inputs(seed: int = 0) -> dict:
    key_of = jax.random.split(jax.random.key(seed), 6)
    tokens = draw_tokens(jax.random.fold_in(key_of[5], 71), 0)
    ln_gain = jnp.clip(1.0 + 0.18 * jax.random.normal(key_of[1], (D,), jnp.float32), 0.1, 1.9)
    w_qkv = draw_w_qkv(jax.random.fold_in(key_of[5], 71), 0)
    q_gain = jnp.clip(jax.random.uniform(key_of[3], (HEAD_DIM,), jnp.float32, 0.7, 2.0), 0.7, 2.0)
    k_gain = jnp.clip(jax.random.uniform(key_of[4], (HEAD_DIM,), jnp.float32, 0.7, 2.0), 0.7, 2.0)
    return {"tokens": tokens, "ln_gain": ln_gain, "w_qkv": w_qkv, "q_gain": q_gain, "k_gain": k_gain}


norm_eps = 1e-06

def layer_norm(values, gain_vector):
    centre = lax.optimization_barrier(jnp.mean(values, axis=-1, keepdims=True))
    centred = values - centre
    spread = lax.optimization_barrier(jnp.mean(centred * centred, axis=-1, keepdims=True))
    return centred * lax.rsqrt(spread + norm_eps) * gain_vector

def to_heads(features):
    leading = features.shape[:-1]
    parted = features.reshape(leading + (SPLITS, HEADS, HEAD_DIM // SPLITS))
    swapped = jnp.moveaxis(parted, -3, -2)
    return swapped.reshape(leading + (HEADS, HEAD_DIM))

def from_heads(features):
    leading = features.shape[:-2]
    parted = features.reshape(leading + (HEADS, SPLITS, HEAD_DIM // SPLITS))
    swapped = jnp.moveaxis(parted, -2, -3)
    return swapped.reshape(leading + (D,))

def reference(tokens, ln_gain, w_qkv, q_gain, k_gain):
    normed = layer_norm(tokens.astype(jnp.float32), ln_gain).astype(jnp.bfloat16)
    projected = jnp.dot(normed, w_qkv.reshape(D, 3 * D), preferred_element_type=jnp.float32).astype(jnp.bfloat16)
    projected = projected.reshape(IMAGES, PATCHES, 3, D)

    def attend(one_image):
        per_head = to_heads(one_image)
        queries = (layer_norm(per_head[:, 0].astype(jnp.float32), q_gain) * HEAD_DIM ** (-0.5)).astype(jnp.bfloat16)
        key_vecs = layer_norm(per_head[:, 1].astype(jnp.float32), k_gain).astype(jnp.bfloat16)
        values = per_head[:, 2]
        scores = jnp.einsum('qhe,khe->hqk', queries.astype(jnp.float32), key_vecs.astype(jnp.float32))
        raised = jnp.exp(scores)
        weights = (raised / lax.optimization_barrier(jnp.sum(raised, axis=-1, keepdims=True))).astype(jnp.bfloat16)
        attended = jnp.einsum('hqk,khe->qhe', weights.astype(jnp.float32), values.astype(jnp.float32)).astype(jnp.bfloat16)
        return from_heads(attended)
    context = lax.map(attend, projected)
    return context.reshape(TOKENS, D)
```

```python
import functools

import jax
import jax.numpy as jnp
from jax import lax
from jax.experimental import pallas as pl
from jax.experimental.pallas import tpu as pltpu
from jax.sharding import PartitionSpec as P

HEADS = 48
HEAD_DIM = 128
PATCHES = 256
SPLITS = 4


norm_eps = 1e-06


def from_behind(shard, axis, by):
    length = lax.axis_size(axis)
    return lax.ppermute(shard, axis, [(i, (i + by) % length) for i in range(length)])


def layer_norm(values, gain_vector):
    centre = jnp.mean(values, axis=-1, keepdims=True)
    centred = values - centre
    spread = jnp.mean(centred * centred, axis=-1, keepdims=True)
    return centred * lax.rsqrt(spread + norm_eps) * gain_vector


def head_norm(pieces, gain_rows):
    values = pieces.astype(jnp.float32)
    centre = jnp.mean(values, axis=(0, 4), keepdims=True)
    centred = values - centre
    spread = jnp.mean(centred * centred, axis=(0, 4), keepdims=True)
    return centred * lax.rsqrt(spread + norm_eps) * gain_rows[:, None, None, None, :]


def ordered_gains(gain_vector, quarter_order):
    gain_table = gain_vector.reshape(SPLITS, -1)
    selector = (quarter_order[:, None] == jnp.arange(SPLITS, dtype=jnp.int32)[None, :]).astype(
        jnp.float32
    )
    return jnp.dot(selector, gain_table, precision=lax.Precision.HIGHEST)


def plain_body(tokens, ln_gain, w_qkv, q_gain, k_gain):
    local_rows = tokens.shape[0]
    normed = layer_norm(tokens.astype(jnp.float32), ln_gain).astype(jnp.bfloat16)
    flat_weight = w_qkv.reshape(w_qkv.shape[0], -1)
    out_width = flat_weight.shape[1]
    row_piece = lax.all_gather(w_qkv, "dp", axis=0, tiled=True)
    partial_value = jnp.dot(
        normed, row_piece.reshape(row_piece.shape[0], out_width), preferred_element_type=jnp.float32
    )
    projected = partial_value.astype(jnp.bfloat16)
    groups = lax.axis_size("mp") // SPLITS
    head_count = HEADS // groups
    quarter_rows = PATCHES // SPLITS
    my_quarter = lax.axis_index("mp") // groups
    images = local_rows // PATCHES
    head_view = projected.reshape(images, PATCHES, 3, head_count, HEAD_DIM // SPLITS)
    queries = head_view[:, :, 0]
    keys_vals = head_view[:, :, 1:]
    counting = jnp.arange(SPLITS, dtype=jnp.int32)
    own_rows = lax.dynamic_slice_in_dim(queries, my_quarter * quarter_rows, quarter_rows, 1)
    query_list = [own_rows]
    pair_list = [keys_vals]
    for offset in range(1, SPLITS):
        outgoing = lax.dynamic_slice_in_dim(
            queries, (my_quarter + offset) % SPLITS * quarter_rows, quarter_rows, 1
        )
        got_query, got_pair = from_behind((outgoing, keys_vals), "mp", offset * groups)
        query_list.append(got_query)
        pair_list.append(got_pair)
    query_pieces = jnp.stack(query_list, 0)
    pair_pieces = jnp.stack(pair_list, 0)
    quarter_order = (my_quarter - counting) % SPLITS
    query_normed = (
        head_norm(query_pieces, ordered_gains(q_gain, quarter_order)) * HEAD_DIM ** (-0.5)
    ).astype(jnp.bfloat16)
    key_normed = head_norm(pair_pieces[:, :, :, 0], ordered_gains(k_gain, quarter_order)).astype(
        jnp.bfloat16
    )
    value_part = pair_pieces[:, :, :, 1]
    scores = jnp.einsum(
        "sirhe,sikhe->ihrk", query_normed, key_normed, preferred_element_type=jnp.float32
    )
    raised = jnp.exp(scores)
    weights = (raised / jnp.sum(raised, axis=-1, keepdims=True)).astype(jnp.bfloat16)
    context = jnp.einsum(
        "ihrk,sikhe->sirhe", weights, value_part, preferred_element_type=jnp.float32
    ).astype(jnp.bfloat16)
    rows_list = [context[0]]
    for offset in range(1, SPLITS):
        wanted = (my_quarter - offset) % SPLITS
        slot_index = jnp.sum(jnp.where(quarter_order == wanted, counting, 0))
        outgoing = lax.dynamic_index_in_dim(context, slot_index, 0, keepdims=False)
        rows_list.append(from_behind(outgoing, "mp", (SPLITS - offset) * groups))
    own_block = jnp.roll(jnp.concatenate(rows_list, 1), my_quarter * quarter_rows, axis=1)
    return own_block.reshape(local_rows, -1)

LANES = 128
CHUNKS = 3
IN_FLIGHT = 3
VMEM_LIMIT = 56 * 1024 * 1024


def shift(value, axis, by):
    length = lax.axis_size(axis)
    return lax.ppermute(value, axis, [(i, (i + by) % length) for i in range(length)])


def to_sibling(value, axis):
    length = lax.axis_size(axis)
    return lax.ppermute(value, axis, [(i, i ^ 1) for i in range(length)])


def after(value, earlier):
    return lax.optimization_barrier((value, earlier))


def project_kernel(dp_size, normed_ref, *refs):
    *weight_refs, out_ref = refs
    me = lax.axis_index("dp")
    sibling = me + 1 - 2 * lax.rem(me, 2)
    depth = weight_refs[0].shape[1]
    total = None
    for slot, weight_ref in enumerate(weight_refs):
        start = (me, sibling)[slot % 2]
        source = lax.rem(start - 2 * (slot // 2) + dp_size, dp_size)
        columns = pl.ds(pl.multiple_of(source * depth, LANES), depth)
        term = jnp.dot(
            normed_ref[:, columns], weight_ref[0], preferred_element_type=jnp.float32
        )
        total = term if total is None else total + term
    out_ref[0] = total.T.astype(out_ref.dtype)


def project(normed, weights):
    dp_size = len(weights)
    kinds, depth, width = weights[0].shape
    rows, features = normed.shape
    block = 256 if width % 256 == 0 else LANES
    return pl.pallas_call(
        functools.partial(project_kernel, dp_size),
        grid=(kinds, width // block),
        out_shape=jax.ShapeDtypeStruct((kinds, width, rows), jnp.bfloat16),
        in_specs=[pl.BlockSpec((rows, features), lambda j, n: (0, 0))]
        + [pl.BlockSpec((1, depth, block), lambda j, n: (j, 0, n))] * dp_size,
        out_specs=pl.BlockSpec((1, block, rows), lambda j, n: (j, n, 0)),
        compiler_params=pltpu.CompilerParams(vmem_limit_bytes=VMEM_LIMIT),
        cost_estimate=pl.CostEstimate(
            flops=2 * rows * features * width * kinds,
            bytes_accessed=2 * (rows * features + kinds * width * (features + rows)),
            transcendentals=0,
        ),
        name="project",
    )(normed, *weights)


def column_norm(pieces, gain_column):
    values = jnp.concatenate(pieces, axis=0).astype(jnp.float32)
    centre = jnp.mean(values, axis=0, keepdims=True)
    centred = values - centre
    spread = jnp.mean(centred * centred, axis=0, keepdims=True)
    return centred * lax.rsqrt(spread + norm_eps) * gain_column


def weights_kernel(q_gain_ref, k_gain_ref, *refs):
    *piece_refs, out_ref = refs
    query = (
        column_norm([ref[0] for ref in piece_refs], q_gain_ref[...]) * HEAD_DIM ** (-0.5)
    ).astype(jnp.bfloat16)
    key = column_norm([ref[1] for ref in piece_refs], k_gain_ref[...]).astype(jnp.bfloat16)
    for image in range(out_ref.shape[1]):
        span = slice(image * PATCHES, (image + 1) * PATCHES)
        scores = lax.dot_general(
            key[:, span],
            query[:, span],
            (((0,), (0,)), ((), ())),
            preferred_element_type=jnp.float32,
        )
        raised = jnp.exp(scores)
        total = jnp.sum(raised, axis=0, keepdims=True)
        out_ref[0, image] = (raised / total).astype(out_ref.dtype)


def softmax_weights(pieces, q_gain_column, k_gain_column):
    _, height, rows = pieces[0].shape
    part = HEAD_DIM // SPLITS
    heads, images = height // part, rows // PATCHES
    whole = pl.BlockSpec((HEAD_DIM, 1), lambda h: (0, 0))
    return pl.pallas_call(
        weights_kernel,
        grid=(heads,),
        out_shape=jax.ShapeDtypeStruct((heads, images, PATCHES, PATCHES), jnp.bfloat16),
        in_specs=[whole, whole] + [pl.BlockSpec((2, part, rows), lambda h: (0, h, 0))] * SPLITS,
        out_specs=pl.BlockSpec((1, images, PATCHES, PATCHES), lambda h: (h, 0, 0, 0)),
        cost_estimate=pl.CostEstimate(
            flops=2 * heads * rows * PATCHES * HEAD_DIM,
            bytes_accessed=4 * heads * rows * (HEAD_DIM + PATCHES),
            transcendentals=heads * rows * PATCHES,
        ),
        name="softmax_weights",
    )(q_gain_column, k_gain_column, *pieces)


def attend_kernel(weights_ref, *refs):
    piece_refs, out_refs = refs[:SPLITS], refs[SPLITS:]
    values = jnp.concatenate([ref[0] for ref in piece_refs], axis=0)
    part = HEAD_DIM // SPLITS
    for image in range(weights_ref.shape[1]):
        span = slice(image * PATCHES, (image + 1) * PATCHES)
        attended = jnp.dot(
            values[:, span], weights_ref[0, image], preferred_element_type=jnp.float32
        ).astype(jnp.bfloat16)
        for slot, out_ref in enumerate(out_refs):
            out_ref[:, span] = attended[slot * part : (slot + 1) * part]


def attend(weights, pieces):
    _, height, rows = pieces[0].shape
    part = HEAD_DIM // SPLITS
    heads, images = weights.shape[:2]
    return pl.pallas_call(
        attend_kernel,
        grid=(heads,),
        out_shape=[jax.ShapeDtypeStruct((height, rows), jnp.bfloat16)] * SPLITS,
        in_specs=[pl.BlockSpec((1, images, PATCHES, PATCHES), lambda h: (h, 0, 0, 0))]
        + [pl.BlockSpec((1, part, rows), lambda h: (0, h, 0))] * SPLITS,
        out_specs=[pl.BlockSpec((part, rows), lambda h: (h, 0))] * SPLITS,
        cost_estimate=pl.CostEstimate(
            flops=2 * heads * rows * PATCHES * HEAD_DIM,
            bytes_accessed=2 * heads * rows * (2 * HEAD_DIM + PATCHES),
            transcendentals=0,
        ),
        name="attend",
    )(weights, *pieces)


def assemble_kernel(groups, *refs):
    *piece_refs, out_ref, upright = refs
    quarter = lax.axis_index("mp") // groups
    height = piece_refs[0].shape[0]
    for place, piece_ref in enumerate(piece_refs):
        chunk, slot = divmod(place, SPLITS)
        owner = lax.rem(quarter + slot, SPLITS)
        row = (chunk * SPLITS + owner) * height
        upright[pl.ds(pl.multiple_of(row, height), height), :] = piece_ref[...]
    out_ref[...] = upright[...].T


def assemble(pieces, groups):
    height, rows = pieces[0].shape
    width = height * len(pieces)
    return pl.pallas_call(
        functools.partial(assemble_kernel, groups),
        out_shape=jax.ShapeDtypeStruct((rows, width), jnp.bfloat16),
        in_specs=[pl.BlockSpec(memory_space=pltpu.VMEM)] * len(pieces),
        out_specs=pl.BlockSpec(memory_space=pltpu.VMEM),
        scratch_shapes=[pltpu.VMEM((width, rows), jnp.bfloat16)],
        name="assemble",
    )(*pieces)


def exchange(columns, quarter, groups):
    height = columns.shape[1] // SPLITS
    pieces = []
    for offset in range(SPLITS):
        target = (quarter + offset) % SPLITS
        piece = lax.dynamic_slice_in_dim(columns, target * height, height, 1)
        pieces.append(shift(piece, "mp", offset * groups) if offset else piece)
    return pieces


def body(tokens, ln_gain, w_qkv, q_gain, k_gain):
    groups = lax.axis_size("mp") // SPLITS
    dp_size = lax.axis_size("dp")
    quarter = lax.axis_index("mp") // groups
    stacked = jnp.transpose(w_qkv, (1, 0, 2))
    width = stacked.shape[2] // CHUNKS
    normed = layer_norm(tokens.astype(jnp.float32), ln_gain).astype(jnp.bfloat16)
    quarter_order = (quarter - jnp.arange(SPLITS, dtype=jnp.int32)) % SPLITS
    q_gain_column = ordered_gains(q_gain, quarter_order).reshape(HEAD_DIM, 1)
    k_gain_column = ordered_gains(k_gain, quarter_order).reshape(HEAD_DIM, 1)
    spans = []
    for chunk in range(CHUNKS):
        columns = slice(chunk * width, (chunk + 1) * width)
        spans += [(slice(0, 2), columns), (slice(2, 3), columns)]
    sent = []

    def send(own):
        sent.append([own] + [shift(own, "dp", 2 * step) for step in range(1, dp_size // 2)])

    for kinds, columns in spans[:IN_FLIGHT]:
        send(stacked[kinds, :, columns])
    returned = []
    latest = normed
    for chunk in range(CHUNKS):
        received = []
        for place in (2 * chunk, 2 * chunk + 1):
            shards = []
            for held in sent[place]:
                shards += [held, to_sibling(held, "dp")]
            normed, latest = after(normed, latest)
            latest = project(normed, shards)
            if place + IN_FLIGHT < len(spans):
                kinds, columns = spans[place + IN_FLIGHT]
                stacked, latest = after(stacked, latest)
                send(stacked[kinds, :, columns])
            received.append(exchange(latest, quarter, groups))
        weights = softmax_weights(received[0], q_gain_column, k_gain_column)
        attended = attend(weights, received[1])
        latest = attended[0]
        for slot, piece in enumerate(attended):
            returned.append(shift(piece, "mp", (SPLITS - slot) * groups) if slot else piece)
    return assemble(returned, groups)


def solution(mesh):
    local_heads = HEADS * SPLITS // mesh.shape["mp"]
    columns = local_heads * (HEAD_DIM // SPLITS)
    fits = columns % (CHUNKS * LANES) == 0 and local_heads % (CHUNKS * SPLITS) == 0
    return jax.shard_map(
        body if fits and mesh.shape["dp"] % 2 == 0 else plain_body,
        mesh=mesh,
        in_specs=(P("dp", None), P(), P("dp", None, "mp"), P(), P()),
        out_specs=P("dp", "mp"),
        check_vma=False,
    )
```

```python
import functools

import jax
import jax.numpy as jnp
from jax import lax
from jax.experimental import pallas as pl
from jax.experimental.pallas import tpu as pltpu
from jax.sharding import PartitionSpec as P


HEADS = 48
HEAD_DIM = 128
PATCHES = 256
SPLITS = 4


norm_eps = 1e-06


def from_behind(shard, axis, by):
    length = lax.axis_size(axis)
    return lax.ppermute(shard, axis, [(i, (i + by) % length) for i in range(length)])


def layer_norm(values, gain_vector):
    centre = jnp.mean(values, axis=-1, keepdims=True)
    centred = values - centre
    spread = jnp.mean(centred * centred, axis=-1, keepdims=True)
    return centred * lax.rsqrt(spread + norm_eps) * gain_vector


def head_norm(pieces, gain_rows):
    values = pieces.astype(jnp.float32)
    centre = jnp.mean(values, axis=(0, 4), keepdims=True)
    centred = values - centre
    spread = jnp.mean(centred * centred, axis=(0, 4), keepdims=True)
    return centred * lax.rsqrt(spread + norm_eps) * gain_rows[:, None, None, None, :]


def ordered_gains(gain_vector, quarter_order):
    gain_table = gain_vector.reshape(SPLITS, -1)
    selector = (quarter_order[:, None] == jnp.arange(SPLITS, dtype=jnp.int32)[None, :]).astype(
        jnp.float32
    )
    return jnp.dot(selector, gain_table, precision=lax.Precision.HIGHEST)


def plain_body(tokens, ln_gain, w_qkv, q_gain, k_gain):
    local_rows = tokens.shape[0]
    normed = layer_norm(tokens.astype(jnp.float32), ln_gain).astype(jnp.bfloat16)
    flat_weight = w_qkv.reshape(w_qkv.shape[0], -1)
    out_width = flat_weight.shape[1]
    row_piece = lax.all_gather(w_qkv, "dp", axis=0, tiled=True)
    partial_value = jnp.dot(
        normed, row_piece.reshape(row_piece.shape[0], out_width), preferred_element_type=jnp.float32
    )
    projected = partial_value.astype(jnp.bfloat16)
    groups = lax.axis_size("mp") // SPLITS
    head_count = HEADS // groups
    quarter_rows = PATCHES // SPLITS
    my_quarter = lax.axis_index("mp") // groups
    images = local_rows // PATCHES
    head_view = projected.reshape(images, PATCHES, 3, head_count, HEAD_DIM // SPLITS)
    queries = head_view[:, :, 0]
    keys_vals = head_view[:, :, 1:]
    counting = jnp.arange(SPLITS, dtype=jnp.int32)
    own_rows = lax.dynamic_slice_in_dim(queries, my_quarter * quarter_rows, quarter_rows, 1)
    query_list = [own_rows]
    pair_list = [keys_vals]
    for offset in range(1, SPLITS):
        outgoing = lax.dynamic_slice_in_dim(
            queries, (my_quarter + offset) % SPLITS * quarter_rows, quarter_rows, 1
        )
        got_query, got_pair = from_behind((outgoing, keys_vals), "mp", offset * groups)
        query_list.append(got_query)
        pair_list.append(got_pair)
    query_pieces = jnp.stack(query_list, 0)
    pair_pieces = jnp.stack(pair_list, 0)
    quarter_order = (my_quarter - counting) % SPLITS
    query_normed = (
        head_norm(query_pieces, ordered_gains(q_gain, quarter_order)) * HEAD_DIM ** (-0.5)
    ).astype(jnp.bfloat16)
    key_normed = head_norm(pair_pieces[:, :, :, 0], ordered_gains(k_gain, quarter_order)).astype(
        jnp.bfloat16
    )
    value_part = pair_pieces[:, :, :, 1]
    scores = jnp.einsum(
        "sirhe,sikhe->ihrk", query_normed, key_normed, preferred_element_type=jnp.float32
    )
    raised = jnp.exp(scores)
    weights = (raised / jnp.sum(raised, axis=-1, keepdims=True)).astype(jnp.bfloat16)
    context = jnp.einsum(
        "ihrk,sikhe->sirhe", weights, value_part, preferred_element_type=jnp.float32
    ).astype(jnp.bfloat16)
    rows_list = [context[0]]
    for offset in range(1, SPLITS):
        wanted = (my_quarter - offset) % SPLITS
        slot_index = jnp.sum(jnp.where(quarter_order == wanted, counting, 0))
        outgoing = lax.dynamic_index_in_dim(context, slot_index, 0, keepdims=False)
        rows_list.append(from_behind(outgoing, "mp", (SPLITS - offset) * groups))
    own_block = jnp.roll(jnp.concatenate(rows_list, 1), my_quarter * quarter_rows, axis=1)
    return own_block.reshape(local_rows, -1)


LANES = 128
CHUNKS = 3
VMEM_LIMIT = 28 * 1024 * 1024


def shift(value, axis, by):
    length = lax.axis_size(axis)
    return lax.ppermute(value, axis, [(i, (i + by) % length) for i in range(length)])


def to_sibling(value, axis):
    length = lax.axis_size(axis)
    return lax.ppermute(value, axis, [(i, i ^ 1) for i in range(length)])


def project_kernel(dp_size, normed_ref, *refs):
    *weight_refs, out_ref = refs
    me = lax.axis_index("dp")
    sibling = me + 1 - 2 * lax.rem(me, 2)
    depth = weight_refs[0].shape[1]
    total = None
    for slot, weight_ref in enumerate(weight_refs):
        start = (me, sibling)[slot % 2]
        source = lax.rem(start - 2 * (slot // 2) + dp_size, dp_size)
        columns = pl.ds(pl.multiple_of(source * depth, LANES), depth)
        term = jnp.dot(
            normed_ref[:, columns], weight_ref[0], preferred_element_type=jnp.float32
        )
        total = term if total is None else total + term
    out_ref[0] = total.T.astype(out_ref.dtype)


def project(normed, weights):
    dp_size = len(weights)
    kinds, depth, width = weights[0].shape
    rows, features = normed.shape
    block = 256 if width % 256 == 0 else LANES
    return pl.pallas_call(
        functools.partial(project_kernel, dp_size),
        grid=(kinds, width // block),
        out_shape=jax.ShapeDtypeStruct((kinds, width, rows), jnp.bfloat16),
        in_specs=[pl.BlockSpec(memory_space=pltpu.VMEM)]
        + [pl.BlockSpec((1, depth, block), lambda j, n: (j, 0, n))] * dp_size,
        out_specs=pl.BlockSpec((1, block, rows), lambda j, n: (j, n, 0)),
        compiler_params=pltpu.CompilerParams(vmem_limit_bytes=VMEM_LIMIT),
        cost_estimate=pl.CostEstimate(
            flops=2 * rows * features * width * kinds,
            bytes_accessed=2 * (rows * features + kinds * width * (features + rows)),
            transcendentals=0,
        ),
        name="project",
    )(normed, *weights)


def column_norm(pieces, gain_column):
    values = jnp.concatenate(pieces, axis=0).astype(jnp.float32)
    centre = jnp.mean(values, axis=0, keepdims=True)
    centred = values - centre
    spread = jnp.mean(centred * centred, axis=0, keepdims=True)
    return centred * lax.rsqrt(spread + norm_eps) * gain_column


def weights_kernel(q_gain_ref, k_gain_ref, *refs):
    *piece_refs, out_ref = refs
    query = (
        column_norm([ref[0] for ref in piece_refs], q_gain_ref[...]) * HEAD_DIM ** (-0.5)
    ).astype(jnp.bfloat16)
    key = column_norm([ref[1] for ref in piece_refs], k_gain_ref[...]).astype(jnp.bfloat16)
    for image in range(out_ref.shape[1]):
        span = slice(image * PATCHES, (image + 1) * PATCHES)
        scores = lax.dot_general(
            key[:, span],
            query[:, span],
            (((0,), (0,)), ((), ())),
            preferred_element_type=jnp.float32,
        )
        raised = jnp.exp(scores)
        total = jnp.sum(raised, axis=0, keepdims=True)
        out_ref[0, image] = (raised / total).astype(out_ref.dtype)


def softmax_weights(pieces, q_gain_column, k_gain_column):
    _, height, rows = pieces[0].shape
    part = HEAD_DIM // SPLITS
    heads, images = height // part, rows // PATCHES
    whole = pl.BlockSpec((HEAD_DIM, 1), lambda h: (0, 0))
    return pl.pallas_call(
        weights_kernel,
        grid=(heads,),
        out_shape=jax.ShapeDtypeStruct((heads, images, PATCHES, PATCHES), jnp.bfloat16),
        in_specs=[whole, whole] + [pl.BlockSpec((2, part, rows), lambda h: (0, h, 0))] * SPLITS,
        out_specs=pl.BlockSpec((1, images, PATCHES, PATCHES), lambda h: (h, 0, 0, 0)),
        cost_estimate=pl.CostEstimate(
            flops=2 * heads * rows * PATCHES * HEAD_DIM,
            bytes_accessed=4 * heads * rows * (HEAD_DIM + PATCHES),
            transcendentals=heads * rows * PATCHES,
        ),
        name="softmax_weights",
    )(q_gain_column, k_gain_column, *pieces)


def attend_kernel(weights_ref, *refs):
    piece_refs, out_refs = refs[:SPLITS], refs[SPLITS:]
    values = jnp.concatenate([ref[0] for ref in piece_refs], axis=0)
    part = HEAD_DIM // SPLITS
    for image in range(weights_ref.shape[1]):
        span = slice(image * PATCHES, (image + 1) * PATCHES)
        attended = jnp.dot(
            values[:, span], weights_ref[0, image], preferred_element_type=jnp.float32
        ).astype(jnp.bfloat16)
        for slot, out_ref in enumerate(out_refs):
            out_ref[:, span] = attended[slot * part : (slot + 1) * part]


def attend(weights, pieces):
    _, height, rows = pieces[0].shape
    part = HEAD_DIM // SPLITS
    heads, images = weights.shape[:2]
    return pl.pallas_call(
        attend_kernel,
        grid=(heads,),
        out_shape=[jax.ShapeDtypeStruct((height, rows), jnp.bfloat16)] * SPLITS,
        in_specs=[pl.BlockSpec((1, images, PATCHES, PATCHES), lambda h: (h, 0, 0, 0))]
        + [pl.BlockSpec((1, part, rows), lambda h: (0, h, 0))] * SPLITS,
        out_specs=[pl.BlockSpec((part, rows), lambda h: (h, 0))] * SPLITS,
        cost_estimate=pl.CostEstimate(
            flops=2 * heads * rows * PATCHES * HEAD_DIM,
            bytes_accessed=2 * heads * rows * (2 * HEAD_DIM + PATCHES),
            transcendentals=0,
        ),
        name="attend",
    )(weights, *pieces)


def assemble_kernel(groups, *refs):
    *piece_refs, out_ref, upright = refs
    quarter = lax.axis_index("mp") // groups
    height = piece_refs[0].shape[0]
    for place, piece_ref in enumerate(piece_refs):
        chunk, slot = divmod(place, SPLITS)
        owner = lax.rem(quarter + slot, SPLITS)
        row = (chunk * SPLITS + owner) * height
        upright[pl.ds(pl.multiple_of(row, height), height), :] = piece_ref[...]
    out_ref[...] = upright[...].T


def assemble(pieces, groups):
    height, rows = pieces[0].shape
    width = height * len(pieces)
    return pl.pallas_call(
        functools.partial(assemble_kernel, groups),
        out_shape=jax.ShapeDtypeStruct((rows, width), jnp.bfloat16),
        in_specs=[pl.BlockSpec(memory_space=pltpu.VMEM)] * len(pieces),
        out_specs=pl.BlockSpec(memory_space=pltpu.VMEM),
        scratch_shapes=[pltpu.VMEM((width, rows), jnp.bfloat16)],
        name="assemble",
    )(*pieces)


def outgoing(columns, quarter):
    height = columns.shape[1] // SPLITS
    return [
        lax.dynamic_slice_in_dim(columns, (quarter + offset) % SPLITS * height, height, 1)
        for offset in range(SPLITS)
    ]


def exchange(pieces, groups):
    received = [pieces[0]]
    for offset in range(1, SPLITS):
        received.append(shift(pieces[offset], "mp", offset * groups))
    return received


def row_norm_kernel(tokens_ref, gain_ref, out_ref):
    values = tokens_ref[...].astype(jnp.float32)
    out_ref[...] = layer_norm(values, gain_ref[...]).astype(out_ref.dtype)


def row_norm(tokens, gain):
    rows, features = tokens.shape
    block = 64 if rows % 64 == 0 else rows
    tile = pl.BlockSpec((block, features), lambda i: (i, 0))
    return pl.pallas_call(
        row_norm_kernel,
        grid=(rows // block,),
        out_shape=jax.ShapeDtypeStruct(tokens.shape, jnp.bfloat16),
        in_specs=[tile, pl.BlockSpec((1, features), lambda i: (0, 0))],
        out_specs=tile,
        cost_estimate=pl.CostEstimate(
            flops=8 * rows * features, bytes_accessed=4 * rows * features, transcendentals=rows
        ),
        name="row_norm",
    )(tokens, gain.reshape(1, features))


def body(tokens, ln_gain, w_qkv, q_gain, k_gain):
    groups = lax.axis_size("mp") // SPLITS
    dp_size = lax.axis_size("dp")
    quarter = lax.axis_index("mp") // groups
    stacked = jnp.transpose(w_qkv, (1, 0, 2))
    width = stacked.shape[2] // CHUNKS
    normed = row_norm(tokens, ln_gain)
    quarter_order = (quarter - jnp.arange(SPLITS, dtype=jnp.int32)) % SPLITS
    q_gain_column = ordered_gains(q_gain, quarter_order).reshape(HEAD_DIM, 1)
    k_gain_column = ordered_gains(k_gain, quarter_order).reshape(HEAD_DIM, 1)
    gathered = []
    for place in range(2 * CHUNKS):
        kinds = slice(2, 3) if place % 2 else slice(0, 2)
        own = stacked[kinds, :, place // 2 * width : (place // 2 + 1) * width]
        shards = []
        for step in range(dp_size // 2):
            held = own
            if step:
                held = shift(own, "dp", 2 * step)
            shards += [held, to_sibling(held, "dp")]
        gathered.append(shards)
    returned = []
    for chunk in range(CHUNKS):
        received = []
        for place in (2 * chunk, 2 * chunk + 1):
            projected = project(normed, gathered[place])
            received.append(exchange(outgoing(projected, quarter), groups))
        weights = softmax_weights(received[0], q_gain_column, k_gain_column)
        attended = attend(weights, received[1])
        for slot, piece in enumerate(attended):
            if slot:
                piece = shift(piece, "mp", (SPLITS - slot) * groups)
            returned.append(piece)
    return assemble(returned, groups)


def solution(mesh):
    local_heads = HEADS * SPLITS // mesh.shape["mp"]
    columns = local_heads * (HEAD_DIM // SPLITS)
    fits = columns % (CHUNKS * LANES) == 0 and local_heads % (CHUNKS * SPLITS) == 0
    fits = fits and mesh.shape["dp"] == 4
    return jax.shard_map(
        body if fits else plain_body,
        mesh=mesh,
        in_specs=(P("dp", None), P(), P("dp", None, "mp"), P(), P()),
        out_specs=P("dp", "mp"),
        check_vma=False,
    )
```
